32 devices in a mesh: energy: 8 (over y, x, core), mom: 4 (over z).
Axes of the slice: x: 2, y: 2, z: 4, core: 2. Of those that a mesh axis runs over, the one named last changes fastest.
Arguments:
- lesser: float32 [4, 8, 4, 4, 2, 128, 128], P(None, 'energy', 'mom'), as said below
- greater: float32 [4, 8, 4, 4, 2, 128, 128], P(None, 'energy', 'mom'), as said below
- hamiltonian: float32 [4, 4, 2, 128, 128], P('mom'), as said below
- coupling: float32 [4, 2, 128, 128], P('mom'), may hold values from -0.25 to 0.25
- shift: int32 [1], replicated, may hold values from 1 to 7
- phonon_weight: float32 [2], replicated, may hold values from 0.1 to 0.5
Outputs:
- lesser_next: float32 [4, 8, 4, 4, 2, 128, 128], P(None, 'energy', 'mom')
- greater_next: float32 [4, 8, 4, 4, 2, 128, 128], P(None, 'energy', 'mom')
- current: float32 [], replicated
The draws below stay inside these ranges and needn't reach their ends.
Inputs may be any that keep to these rules, and one draw needn't show every extreme that they name: `lesser`: in each block the complex matrix is i times a Hermitian positive definite matrix. `greater`: in each block the complex matrix is -i times a Hermitian positive definite matrix. `hamiltonian`: each block is Hermitian: real part symmetric, imaginary part antisymmetric.
All inputs are finite; a program needn't handle non-finite values.
Results may differ from the reference program's by a relative error of at most 0.0001.
Values sent between devices are 32-bit elements; how exact they have to be, the bound alone decides.
A program may use at most 128 MiB of HBM per device.

```python
import math
import jax
import jax.numpy as jnp
from jax import lax

B = 128
S = 4
E_DEV = 4
SMAX = 7
NE = 32
NK = 4
N_ENERGY = 8


def occupied(key, sign):
    parts = jax.random.split(key, 3)
    leading = (E_DEV, NE // E_DEV, NK, S)
    real = jax.random.normal(parts[0], leading + (B, B), jnp.float32)
    imag = jax.random.normal(parts[1], leading + (B, B), jnp.float32)
    scale = 1.0 / (2.0 * B)
    herm_re = (jnp.einsum('...ij,...kj->...ik', real, real, precision=lax.Precision.HIGHEST) + jnp.einsum('...ij,...kj->...ik', imag, imag, precision=lax.Precision.HIGHEST)) * scale
    herm_im = (jnp.einsum('...ij,...kj->...ik', imag, real, precision=lax.Precision.HIGHEST) - jnp.einsum('...ij,...kj->...ik', real, imag, precision=lax.Precision.HIGHEST)) * scale
    diagonal = jax.random.uniform(parts[2], leading + (B,), jnp.float32, 0.2, 1.0)
    herm_re = herm_re + diagonal[..., None] * jnp.eye(B, dtype=jnp.float32)
    return jnp.stack([-sign * herm_im, sign * herm_re], 4)


def draw_lesser(key, part):
    return occupied(jax.random.fold_in(key, 11), 1.0)


def draw_greater(key, part):
    return occupied(jax.random.fold_in(key, 12), -1.0)


def draw_hamiltonian(key, part):
    parts = jax.random.split(jax.random.fold_in(key, 13), 3)
    shape = (NK, S, B, B)
    spread = 0.5 / B ** 0.5
    real = jax.random.normal(parts[0], shape, jnp.float32) * spread
    imag = jax.random.normal(parts[1], shape, jnp.float32) * spread
    onsite = jax.random.uniform(parts[2], (NK, S, B), jnp.float32, -1.0, 1.0)
    real = real + jnp.swapaxes(real, -1, -2) + onsite[..., None] * jnp.eye(B, dtype=jnp.float32)
    imag = imag - jnp.swapaxes(imag, -1, -2)
    return jnp.stack([real, imag], 2)


def shard_levels(rng, shape, shards, least, largest):
    gain = 1.0
    for dim, blocks in shards:
        draws = jax.random.uniform(jax.random.fold_in(jax.random.fold_in(rng, 6), dim), (blocks,), jnp.float32, least / len(shards), largest / len(shards))
        gain = gain * jnp.repeat(jnp.exp(draws), shape[dim] // blocks).reshape((-1,) + (1,) * (len(shape) - 1 - dim))
    return gain


def noise(own_key, shape, scale, bound, shards=(), held_as=jnp.bfloat16):
    loudness = shard_levels(own_key, shape, shards, -0.22, 0.18) if shards else 1.0
    values = jax.random.normal(own_key, shape, jnp.float32) * scale * loudness
    return jnp.minimum(jnp.maximum(values, -bound), bound).astype(held_as)


def setup_inputs(seed: int = 0) -> dict:
    key_list = jax.random.split(jax.random.key(seed), 7)
    return {
        "lesser": draw_lesser(jax.random.fold_in(key_list[6], 71), 0),
        "greater": draw_greater(jax.random.fold_in(key_list[6], 71), 0),
        "hamiltonian": draw_hamiltonian(jax.random.fold_in(key_list[6], 71), 0),
        "coupling": noise(key_list[3], (NK, 2, B, B), (4 * B) ** -0.5, 0.25, ((0, 4),), jnp.float32),
        "shift": jax.random.randint(key_list[4], (1,), 1, SMAX + 1).astype(jnp.int32),
        "phonon_weight": jnp.clip(jnp.exp(jax.random.uniform(key_list[5], (2,), jnp.float32, math.log(0.1), math.log(0.5))), 0.1, 0.5),
    }


broaden = 0.2
contact_rate = 0.5
left_level = 0.3
right_level = -0.3
thermal = 0.1
band_edge = 2.0
precise = lax.Precision.HIGHEST

def product(left, right):
    return jnp.einsum('...ij,...jk->...ik', left, right, precision=precise)

def cmul(left, right):
    return (product(left[0], right[0]) - product(left[1], right[1]), product(left[0], right[1]) + product(left[1], right[0]))

def dagger(value):
    return (jnp.swapaxes(value[0], -1, -2), -jnp.swapaxes(value[1], -1, -2))

def sandwich(outer, inner):
    return cmul(cmul(outer, inner), dagger(outer))

def invert(matrix):
    real, imag = matrix
    width = real.shape[-1]
    kernel = jnp.concatenate([jnp.concatenate([real, -imag], -1), jnp.concatenate([imag, real], -1)], -2)
    normal = product(jnp.swapaxes(kernel, -1, -2), kernel)
    lower = jnp.linalg.cholesky(normal)
    rhs = jnp.concatenate([jnp.swapaxes(real, -1, -2), -jnp.swapaxes(imag, -1, -2)], -2)
    middle = jax.scipy.linalg.solve_triangular(lower, rhs, lower=True)
    result = jax.scipy.linalg.solve_triangular(lower, middle, lower=True, trans=1)
    guess = (result[..., :width, :], result[..., width:, :])
    check = cmul(matrix, guess)
    eye = jnp.eye(width, dtype=jnp.float32)
    return cmul(guess, (2.0 * eye - check[0], -check[1]))

def transport(energy, hamiltonian, coupling, sig_less, sig_great):
    slabs = hamiltonian.shape[1]
    width = hamiltonian.shape[-1]
    eye = jnp.eye(width, dtype=jnp.float32)
    level = energy[:, None, None]
    hop = (coupling[:, 0], coupling[:, 1])
    hop_back = dagger(hop)
    fill_left = jax.nn.sigmoid((left_level - energy) / thermal)
    fill_right = jax.nn.sigmoid((right_level - energy) / thermal)
    forward_r = []
    forward_l = []
    for slab in range(slabs):
        less_re = sig_less[:, slab, 0]
        less_im = sig_less[:, slab, 1]
        system_re = level * eye - hamiltonian[:, slab, 0] - 0.5 * (sig_great[:, slab, 0] - less_re)
        system_im = broaden * eye - hamiltonian[:, slab, 1] - 0.5 * (sig_great[:, slab, 1] - less_im)
        inject_re = less_re
        inject_im = less_im
        if slab == 0 or slab == slabs - 1:
            filling = fill_left if slab == 0 else fill_right
            system_im = system_im + contact_rate * eye
            inject_im = inject_im + 2.0 * contact_rate * filling[:, None, None] * eye
        if slab > 0:
            folded = sandwich(hop, forward_r[-1])
            system_re = system_re - folded[0]
            system_im = system_im - folded[1]
            carried = sandwich(hop, forward_l[-1])
            inject_re = inject_re + carried[0]
            inject_im = inject_im + carried[1]
        green = invert((system_re, system_im))
        forward_r.append(green)
        forward_l.append(sandwich(green, (inject_re, inject_im)))
    full_r = forward_r[-1]
    full_l = forward_l[-1]
    outs_r = [full_r]
    outs_l = [full_l]
    for slab in range(slabs - 2, -1, -1):
        green = forward_r[slab]
        green_l = forward_l[slab]
        lead = cmul(green, hop_back)
        spread = cmul(lead, full_r)
        tail = cmul(hop, green)
        extra = cmul(spread, tail)
        new_r = (green[0] + extra[0], green[1] + extra[1])
        cross = cmul(spread, cmul(hop, green_l))
        inner = sandwich(lead, full_l)
        cross_d = dagger(cross)
        new_l = (green_l[0] + inner[0] + cross[0] - cross_d[0], green_l[1] + inner[1] + cross[1] - cross_d[1])
        full_r = new_r
        full_l = new_l
        outs_r.insert(0, full_r)
        outs_l.insert(0, full_l)
    less_blocks = jnp.stack([jnp.stack([value[0], value[1]], 1) for value in outs_l], 1)
    great_blocks = jnp.stack([jnp.stack([outs_l[k][0] + outs_r[k][0] - jnp.swapaxes(outs_r[k][0], -1, -2), outs_l[k][1] + outs_r[k][1] + jnp.swapaxes(outs_r[k][1], -1, -2)], 1) for k in range(slabs)], 1)
    great_trace = jnp.trace(great_blocks[:, 0, 1], axis1=-2, axis2=-1)
    less_trace = jnp.trace(less_blocks[:, 0, 1], axis1=-2, axis2=-1)
    flowing = -(2.0 * contact_rate * fill_left * great_trace + 2.0 * contact_rate * (1.0 - fill_left) * less_trace)
    return (less_blocks, great_blocks, flowing)

def reference(lesser, greater, hamiltonian, coupling, shift, phonon_weight):
    total = E_DEV * N_ENERGY
    tail_shape = (S, 2, B, B)
    mean_less = (jnp.sum(lesser, axis=2) / NK).reshape((total,) + tail_shape)
    mean_great = (jnp.sum(greater, axis=2) / NK).reshape((total,) + tail_shape)
    amount = shift[0].astype(jnp.int32)
    blank = jnp.zeros((SMAX,) + tail_shape, jnp.float32)

    def moved(field, offset):
        padded = jnp.concatenate([blank, field, blank], 0)
        return lax.dynamic_slice_in_dim(padded, (SMAX + offset).astype(jnp.int32), total, 0)
    emission = phonon_weight[0]
    absorption = phonon_weight[1]
    sig_less = emission * moved(mean_less, amount) + absorption * moved(mean_less, -amount)
    sig_great = emission * moved(mean_great, -amount) + absorption * moved(mean_great, amount)
    grid = (jnp.arange(total).astype(jnp.float32) + 0.5) * (2.0 * band_edge / total) - band_edge

    def solve_one(items):
        energy, one_less, one_great = items
        energies = jnp.broadcast_to(energy, (NK,))
        less_wide = jnp.broadcast_to(one_less, (NK,) + tail_shape)
        great_wide = jnp.broadcast_to(one_great, (NK,) + tail_shape)
        return transport(energies, hamiltonian, coupling, less_wide, great_wide)
    less_new, great_new, flowing = lax.map(solve_one, (grid, sig_less, sig_great))
    full_shape = (E_DEV, N_ENERGY, NK) + tail_shape
    current = jnp.sum(flowing) * (2.0 * band_edge / total)
    return (less_new.reshape(full_shape), great_new.reshape(full_shape), current)
```

```python
import functools
import math

import jax
import jax.numpy as jnp
from jax import lax
from jax.experimental import pallas as pl
from jax.experimental.pallas import tpu as pltpu
from jax.sharding import PartitionSpec as P

SMAX = 7

broaden = 0.2
contact_rate = 0.5
left_level = 0.3
right_level = -0.3
thermal = 0.1
band_edge = 2.0


def step_thresholds(count):
    bound = 1.0 - 3e-7
    out = [bound]
    for _ in range(count):
        root = math.sqrt(1.0 - bound)
        bound = (1.0 - root) / (1.0 + root)
        out.append(bound)
    return out


THRESHOLDS = step_thresholds(24)


def split(x):
    high = x.astype(jnp.bfloat16)
    low = (x - high.astype(jnp.float32)).astype(jnp.bfloat16)
    return high, low


def as_left(x):
    high, low = split(x)
    return jnp.concatenate([high, high, low], 1)


def as_right(x):
    width = x.shape[0]
    high, low = split(x)

    def block(t):
        return jnp.concatenate([t, jnp.concatenate([-t[:, width:], t[:, :width]], 1)], 0)

    wide = block(high)
    return jnp.concatenate([wide, block(low), wide], 0)


def mul(left, right):
    return jnp.dot(left, right, preferred_element_type=jnp.float32)


def dagger(x):
    width = x.shape[0]
    return jnp.concatenate([x[:, :width].T, -x[:, width:].T], 1)


def transport_kernel(
    scal, sig, ham, hop, less, great, flow, gr, gl, tg, tl, mat, mleft, cur, curl, cleft, cright
):
    count, slabs = less.shape[0], less.shape[1]
    width = less.shape[-1]
    row = lax.broadcasted_iota(jnp.int32, (width, width), 0)
    col = lax.broadcasted_iota(jnp.int32, (width, width), 1)
    eye = jnp.where(row == col, 1.0, 0.0).astype(jnp.float32)
    wrow = lax.broadcasted_iota(jnp.int32, (width, 2 * width), 0)
    wcol = lax.broadcasted_iota(jnp.int32, (width, 2 * width), 1)
    weye = jnp.where(wrow == wcol, 1.0, 0.0).astype(jnp.float32)

    def opened(packed):
        turned = packed.T
        imag = jnp.where(row >= col, packed, turned)
        real = jnp.where(row < col, packed, jnp.where(row > col, -turned, 0.0))
        return real, imag

    coup = jnp.concatenate([hop[0], hop[1]], 1)
    cleft[...] = as_left(coup)
    cright[...] = as_right(dagger(coup))

    def forward(s, carry):
        first = s == 0
        last = s == slabs - 1
        edge = jnp.where(jnp.logical_or(first, last), contact_rate, 0.0)
        for j in range(count):
            fill = jnp.where(first, scal[1, j], jnp.where(last, scal[2, j], 0.0))
            low = sig[0, j, s]
            d_re, d_im = opened(0.5 * (sig[1, j, s] - low))
            l_re, l_im = opened(low)
            mat[j, :, :width] = scal[0, j] * eye - ham[s, 0] - d_re
            mat[j, :, width:] = (broaden + edge) * eye - ham[s, 1] - d_im
            gl[s, j, :, :width] = l_re
            gl[s, j, :, width:] = l_im + (2.0 * contact_rate) * fill * eye

        @pl.when(s > 0)
        def _():
            for j in range(count):
                lead = mul(cleft[...], as_right(gr[s - 1, j]))
                tg[s - 1, j] = lead
                mat[j] = mat[j] - mul(as_left(lead), cright[...])
                lead = mul(cleft[...], as_right(gl[s - 1, j]))
                tl[s - 1, j] = lead
                gl[s, j] = gl[s, j] + mul(as_left(lead), cright[...])

        lower = None
        for j in range(count):
            m = mat[j]
            left = as_left(m)
            mleft[j] = left
            mh = dagger(m)
            norm = mul(left, as_right(mh))
            top = jnp.max(jnp.max(jnp.abs(norm), axis=1, keepdims=True), axis=0, keepdims=True)
            scaled = norm / top
            square = jnp.sum(jnp.sum(scaled * scaled, axis=1, keepdims=True), axis=0, keepdims=True)
            bound = top * jnp.sqrt(square) * 1.0001
            mat[j] = norm / bound
            cur[j] = mh / bound
            this = (0.98 * broaden * broaden) / bound
            lower = this if lower is None else jnp.minimum(lower, this)
        level = lower[0, 0]
        steps = jnp.int32(0)
        for threshold in THRESHOLDS[:-1]:
            steps = steps + jnp.where(level < threshold, 1, 0).astype(jnp.int32)
        lane = jnp.broadcast_to(lower, (1, 2 * width))

        def advance(j, prod, l):
            mu = 2.0 / (1.0 + l)
            gap = weye - mu * prod
            now = cur[j]
            cur[j] = mu * (now + mul(as_left(now), as_right(gap)))

        for j in range(count):
            advance(j, mat[j], lane)

        def newton(k, l):
            prods = [mul(mleft[j], as_right(cur[j])) for j in range(count)]
            for j in range(count):
                advance(j, prods[j], l)
            return jnp.minimum(4.0 * l / ((1.0 + l) * (1.0 + l)), 1.0)

        lane = jnp.minimum(4.0 * lane / ((1.0 + lane) * (1.0 + lane)), 1.0)
        lax.fori_loop(1, steps, newton, lane)
        for j in range(count):
            green = cur[j]
            gr[s, j] = green
            half = mul(as_left(green), as_right(gl[s, j]))
            gl[s, j] = mul(as_left(half), as_right(dagger(green)))
        return carry

    lax.fori_loop(0, slabs, forward, 0)

    def emit(s, j, full_r, full_l):
        l_re, l_im = full_l[:, :width], full_l[:, width:]
        r_re, r_im = full_r[:, :width], full_r[:, width:]
        less[j, s, 0] = l_re
        less[j, s, 1] = l_im
        great[j, s, 0] = l_re + r_re - r_re.T
        great[j, s, 1] = l_im + r_im + r_im.T

    for j in range(count):
        curl[j] = gl[slabs - 1, j]
        emit(slabs - 1, j, cur[j], curl[j])

    def backward(i, carry):
        s = slabs - 2 - i
        for j in range(count):
            green = gr[s, j]
            lead = mul(as_left(green), cright[...])
            uleft = as_left(lead)
            spread = as_left(mul(uleft, as_right(cur[j])))
            new_r = green + mul(spread, as_right(tg[s, j]))
            cross = mul(spread, as_right(tl[s, j]))
            inner = mul(as_left(mul(uleft, as_right(curl[j]))), as_right(dagger(lead)))
            new_l = gl[s, j] + inner + cross - dagger(cross)
            cur[j] = new_r
            curl[j] = new_l
            emit(s, j, new_r, new_l)
        return carry

    lax.fori_loop(0, slabs - 1, backward, 0)
    total = jnp.zeros((1, width), jnp.float32)
    for j in range(count):
        fill = scal[1, j]
        mix = fill * great[j, 0, 1] + (1.0 - fill) * less[j, 0, 1]
        total = total - jnp.sum(jnp.where(row == col, mix, 0.0), axis=0, keepdims=True)
    flow[...] = (2.0 * contact_rate) * total


def transport(scal, sig, ham, hop):
    count, slabs, width = sig.shape[1], sig.shape[2], sig.shape[-1]
    wide = (count, width, 2 * width)
    vmem = pl.BlockSpec(memory_space=pltpu.VMEM)
    block = jax.ShapeDtypeStruct((count, slabs, 2, width, width), jnp.float32)
    return pl.pallas_call(
        transport_kernel,
        out_shape=(block, block, jax.ShapeDtypeStruct((1, width), jnp.float32)),
        in_specs=[pl.BlockSpec(memory_space=pltpu.SMEM), vmem, vmem, vmem],
        out_specs=(vmem, vmem, vmem),
        scratch_shapes=[
            pltpu.VMEM((slabs,) + wide, jnp.float32),
            pltpu.VMEM((slabs,) + wide, jnp.float32),
            pltpu.VMEM((slabs,) + wide, jnp.float32),
            pltpu.VMEM((slabs,) + wide, jnp.float32),
            pltpu.VMEM(wide, jnp.float32),
            pltpu.VMEM((count, width, 6 * width), jnp.bfloat16),
            pltpu.VMEM(wide, jnp.float32),
            pltpu.VMEM(wide, jnp.float32),
            pltpu.VMEM((width, 6 * width), jnp.bfloat16),
            pltpu.VMEM((6 * width, 2 * width), jnp.bfloat16),
        ],
        compiler_params=pltpu.CompilerParams(vmem_limit_bytes=48 * 1024 * 1024),
        name="transport",
    )(scal, sig, ham, hop)


def rotated(array, axis, by):
    size = lax.axis_size(axis)
    if by % size == 0:
        return array
    return lax.ppermute(array, axis, [(i, (i + by) % size) for i in range(size)])


def moved(field, by):
    count = field.shape[1]
    by = max(-count, min(count, by))
    blank = jnp.zeros_like(field[:, : abs(by)])
    if by > 0:
        return jnp.concatenate([field[:, by:], blank], 1)
    if by < 0:
        return jnp.concatenate([blank, field[:, :by]], 1)
    return field


def exchanged(amount, mean):
    n_energy = lax.axis_size("energy")
    here = lax.axis_index("energy")
    turns, rest = divmod(amount, n_energy)
    above = rotated(mean, "energy", -rest)
    below = rotated(mean, "energy", rest)
    upper = jnp.where(here + rest >= n_energy, moved(above, turns + 1), moved(above, turns))
    under = jnp.where(here - rest < 0, moved(below, -turns - 1), moved(below, -turns))
    return upper, under


def shards(lesser, greater, hamiltonian, coupling, shift, phonon_weight):
    n_energy = lax.axis_size("energy")
    n_mom = lax.axis_size("mom")
    here = lax.axis_index("energy")
    mine = lax.axis_index("mom")
    per_dev, slabs, width = lesser.shape[0], lesser.shape[3], lesser.shape[-1]
    total = per_dev * n_energy
    part = slabs // n_mom
    row = lax.broadcasted_iota(jnp.int32, (width, width), 0)
    col = lax.broadcasted_iota(jnp.int32, (width, width), 1)

    def share(owner):
        def packed(x):
            x = lax.dynamic_slice_in_dim(x[:, 0, 0], owner * part, part, 1)
            return jnp.where(row >= col, x[:, :, 1], x[:, :, 0])

        return jnp.stack([packed(lesser), packed(greater)], 0)

    arrived = [
        rotated(share((mine + k) % n_mom), "mom", k) for k in range(1, n_mom)
    ]
    mean = share(mine)
    for piece in arrived:
        mean = mean + piece
    mean = mean / n_mom
    upper, beneath = lax.switch(
        jnp.clip(shift[0] - 1, 0, SMAX - 1),
        [functools.partial(exchanged, p) for p in range(1, SMAX + 1)],
        mean,
    )
    emission = phonon_weight[0]
    absorption = phonon_weight[1]
    own = jnp.stack(
        [
            emission * upper[0] + absorption * beneath[0],
            emission * beneath[1] + absorption * upper[1],
        ],
        0,
    )
    sig = jnp.zeros((2, per_dev, slabs, width, width), jnp.float32)
    sig = lax.dynamic_update_slice_in_dim(sig, own, mine * part, 2)
    for k in range(1, n_mom):
        piece = rotated(own, "mom", k)
        sig = lax.dynamic_update_slice_in_dim(sig, piece, ((mine - k) % n_mom) * part, 2)
    grid = (jnp.arange(per_dev) * n_energy + here).astype(jnp.float32)
    energy = (grid + 0.5) * (2.0 * band_edge / total) - band_edge
    scal = jnp.stack(
        [
            energy,
            jax.nn.sigmoid((left_level - energy) / thermal),
            jax.nn.sigmoid((right_level - energy) / thermal),
        ],
        0,
    )
    less_new, great_new, flowing = transport(scal, sig, hamiltonian[0], coupling[0])
    partial_flow = jnp.sum(flowing) * (2.0 * band_edge / total)
    current = lax.psum(partial_flow, ("energy", "mom"))
    return (less_new[:, None, None], great_new[:, None, None], current)


def solution(mesh):
    block = P(None, "energy", "mom", None, None, None, None)
    return jax.shard_map(
        shards,
        mesh=mesh,
        in_specs=(block, block, P("mom"), P("mom"), P(), P()),
        out_specs=(block, block, P()),
        check_vma=False,
    )
```

```python
import functools
import math

import jax
import jax.numpy as jnp
from jax import lax
from jax.experimental import pallas as pl
from jax.experimental.pallas import tpu as pltpu
from jax.sharding import PartitionSpec as P


SMAX = 7

broaden = 0.2
contact_rate = 0.5
left_level = 0.3
right_level = -0.3
thermal = 0.1
band_edge = 2.0


def step_thresholds(count):
    bound = 1.0 - 3e-7
    out = [bound]
    for _ in range(count):
        root = math.sqrt(1.0 - bound)
        bound = (1.0 - root) / (1.0 + root)
        out.append(bound)
    return out


THRESHOLDS = step_thresholds(24)


def split(x):
    high = x.astype(jnp.bfloat16)
    low = (x - high.astype(jnp.float32)).astype(jnp.bfloat16)
    return high, low


def as_left(x):
    high, low = split(x)
    return jnp.concatenate([high, high, low], 1)


def as_right(x):
    width = x.shape[0]
    high, low = split(x)

    def block(t):
        return jnp.concatenate([t, jnp.concatenate([-t[:, width:], t[:, :width]], 1)], 0)

    wide = block(high)
    return jnp.concatenate([wide, block(low), wide], 0)


def mul(left, right):
    return jnp.dot(left, right, preferred_element_type=jnp.float32)


def dagger(x):
    width = x.shape[0]
    return jnp.concatenate([x[:, :width].T, -x[:, width:].T], 1)


def transport_kernel(
    scal, sig_l, sig_g, ham, hop, less, great, flow, gr, gl, tg, tl, mat, mleft, cur, curl, cleft, cright
):
    count, slabs = less.shape[0], less.shape[1]
    width = less.shape[-1]
    row = lax.broadcasted_iota(jnp.int32, (width, width), 0)
    col = lax.broadcasted_iota(jnp.int32, (width, width), 1)
    eye = jnp.where(row == col, 1.0, 0.0).astype(jnp.float32)
    wrow = lax.broadcasted_iota(jnp.int32, (width, 2 * width), 0)
    wcol = lax.broadcasted_iota(jnp.int32, (width, 2 * width), 1)
    weye = jnp.where(wrow == wcol, 1.0, 0.0).astype(jnp.float32)

    def opened(packed):
        turned = packed.T
        imag = jnp.where(row >= col, packed, turned)
        real = jnp.where(row < col, packed, jnp.where(row > col, -turned, 0.0))
        return real, imag

    coup = jnp.concatenate([hop[0], hop[1]], 1)
    cleft[...] = as_left(coup)
    cright[...] = as_right(dagger(coup))

    def forward(s, carry):
        first = s == 0
        last = s == slabs - 1
        edge = jnp.where(jnp.logical_or(first, last), contact_rate, 0.0)
        for j in range(count):
            fill = jnp.where(first, scal[1, j], jnp.where(last, scal[2, j], 0.0))
            low = sig_l[j, s]
            d_re, d_im = opened(0.5 * (sig_g[j, s] - low))
            l_re, l_im = opened(low)
            mat[j, :, :width] = scal[0, j] * eye - ham[s, 0] - d_re
            mat[j, :, width:] = (broaden + edge) * eye - ham[s, 1] - d_im
            gl[s, j, :, :width] = l_re
            gl[s, j, :, width:] = l_im + (2.0 * contact_rate) * fill * eye

        @pl.when(s > 0)
        def _():
            for j in range(count):
                lead = mul(cleft[...], as_right(gr[s - 1, j]))
                tg[s - 1, j] = lead
                mat[j] = mat[j] - mul(as_left(lead), cright[...])
                lead = mul(cleft[...], as_right(gl[s - 1, j]))
                tl[s - 1, j] = lead
                gl[s, j] = gl[s, j] + mul(as_left(lead), cright[...])

        lower = None
        for j in range(count):
            m = mat[j]
            left = as_left(m)
            mleft[j] = left
            mh = dagger(m)
            norm = mul(left, as_right(mh))
            top = jnp.max(jnp.max(jnp.abs(norm), axis=1, keepdims=True), axis=0, keepdims=True)
            scaled = norm / top
            square = jnp.sum(jnp.sum(scaled * scaled, axis=1, keepdims=True), axis=0, keepdims=True)
            bound = top * jnp.sqrt(square) * 1.0001
            mat[j] = norm / bound
            cur[j] = mh / bound
            this = (0.98 * broaden * broaden) / bound
            lower = this if lower is None else jnp.minimum(lower, this)
        level = lower[0, 0]
        steps = jnp.int32(0)
        for threshold in THRESHOLDS[:-1]:
            steps = steps + jnp.where(level < threshold, 1, 0).astype(jnp.int32)
        lane = jnp.broadcast_to(lower, (1, 2 * width))

        def advance(j, prod, l):
            mu = 2.0 / (1.0 + l)
            gap = weye - mu * prod
            now = cur[j]
            cur[j] = mu * (now + mul(as_left(now), as_right(gap)))

        for j in range(count):
            advance(j, mat[j], lane)

        def newton(k, l):
            prods = [mul(mleft[j], as_right(cur[j])) for j in range(count)]
            for j in range(count):
                advance(j, prods[j], l)
            return jnp.minimum(4.0 * l / ((1.0 + l) * (1.0 + l)), 1.0)

        lane = jnp.minimum(4.0 * lane / ((1.0 + lane) * (1.0 + lane)), 1.0)
        lax.fori_loop(1, steps, newton, lane)
        for j in range(count):
            green = cur[j]
            gr[s, j] = green
            half = mul(as_left(green), as_right(gl[s, j]))
            gl[s, j] = mul(as_left(half), as_right(dagger(green)))
        return carry

    lax.fori_loop(0, slabs, forward, 0)

    def emit(s, j, full_r, full_l):
        l_re, l_im = full_l[:, :width], full_l[:, width:]
        r_re, r_im = full_r[:, :width], full_r[:, width:]
        less[j, s, 0] = l_re
        less[j, s, 1] = l_im
        great[j, s, 0] = l_re + r_re - r_re.T
        great[j, s, 1] = l_im + r_im + r_im.T

    for j in range(count):
        curl[j] = gl[slabs - 1, j]
        emit(slabs - 1, j, cur[j], curl[j])

    def backward(i, carry):
        s = slabs - 2 - i
        for j in range(count):
            green = gr[s, j]
            lead = mul(as_left(green), cright[...])
            uleft = as_left(lead)
            spread = as_left(mul(uleft, as_right(cur[j])))
            new_r = green + mul(spread, as_right(tg[s, j]))
            cross = mul(spread, as_right(tl[s, j]))
            inner = mul(as_left(mul(uleft, as_right(curl[j]))), as_right(dagger(lead)))
            new_l = gl[s, j] + inner + cross - dagger(cross)
            cur[j] = new_r
            curl[j] = new_l
            emit(s, j, new_r, new_l)
        return carry

    lax.fori_loop(0, slabs - 1, backward, 0)
    total = jnp.zeros((1, width), jnp.float32)
    for j in range(count):
        fill = scal[1, j]
        mix = fill * great[j, 0, 1] + (1.0 - fill) * less[j, 0, 1]
        total = total - jnp.sum(jnp.where(row == col, mix, 0.0), axis=0, keepdims=True)
    flow[...] = jnp.broadcast_to((2.0 * contact_rate) * total, flow.shape)


def transport(scal, sig_l, sig_g, ham, hop):
    count, slabs, width = sig_l.shape[0], sig_l.shape[1], sig_l.shape[-1]
    wide = (count, width, 2 * width)
    vmem = pl.BlockSpec(memory_space=pltpu.VMEM)
    block = jax.ShapeDtypeStruct((count, slabs, 2, width, width), jnp.float32)
    return pl.pallas_call(
        transport_kernel,
        out_shape=(block, block, jax.ShapeDtypeStruct((8, width), jnp.float32)),
        in_specs=[pl.BlockSpec(memory_space=pltpu.SMEM), vmem, vmem, vmem, vmem],
        out_specs=(vmem, vmem, vmem),
        scratch_shapes=[
            pltpu.VMEM((slabs,) + wide, jnp.float32),
            pltpu.VMEM((slabs,) + wide, jnp.float32),
            pltpu.VMEM((slabs,) + wide, jnp.float32),
            pltpu.VMEM((slabs,) + wide, jnp.float32),
            pltpu.VMEM(wide, jnp.float32),
            pltpu.VMEM((count, width, 6 * width), jnp.bfloat16),
            pltpu.VMEM(wide, jnp.float32),
            pltpu.VMEM(wide, jnp.float32),
            pltpu.VMEM((width, 6 * width), jnp.bfloat16),
            pltpu.VMEM((6 * width, 2 * width), jnp.bfloat16),
        ],
        compiler_params=pltpu.CompilerParams(vmem_limit_bytes=48 * 1024 * 1024),
        name="transport",
    )(scal, sig_l, sig_g, ham, hop)


def sum_kernel(n_energy, n_mom, scale, flow, out, rows, table, local, send, recv):
    here = lax.axis_index("energy")
    mine = lax.axis_index("mom")
    moms = [lax.rem(mine + k, n_mom) for k in range(1, n_mom)]
    energies = [lax.rem(here + k, n_energy) for k in range(1, n_energy)]
    barrier = pltpu.get_barrier_semaphore()
    for m in moms:
        pl.semaphore_signal(
            barrier, inc=1, device_id=(here, m), device_id_type=pl.DeviceIdType.MESH
        )
    for e in energies:
        pl.semaphore_signal(
            barrier, inc=1, device_id=(e, mine), device_id_type=pl.DeviceIdType.MESH
        )
    pl.semaphore_wait(barrier, n_mom + n_energy - 2)

    def spread(src, dst, base, devices):
        copies = []
        for k, device in enumerate(devices):
            copy = pltpu.make_async_remote_copy(
                src_ref=src,
                dst_ref=dst,
                send_sem=send.at[base + k],
                recv_sem=recv.at[base + k],
                device_id=device,
                device_id_type=pl.DeviceIdType.MESH,
            )
            copy.start()
            copies.append(copy)
        own = pltpu.make_async_copy(src, dst, local)
        own.start()
        own.wait()
        for copy in copies:
            copy.wait()

    spread(flow, rows.at[mine], 0, [(here, m) for m in moms])
    spread(rows, table.at[here], n_mom - 1, [(e, mine) for e in energies])
    total = jnp.sum(table[...].reshape(n_energy * n_mom * 8, -1), axis=0, keepdims=True)
    total = jnp.sum(total, axis=1, keepdims=True) * (scale / 8.0)
    out[...] = jnp.broadcast_to(total, out.shape)


def summed(flow, scale):
    n_energy, n_mom = lax.axis_size("energy"), lax.axis_size("mom")
    copies = n_energy + n_mom - 2
    vmem = pl.BlockSpec(memory_space=pltpu.VMEM)
    return pl.pallas_call(
        functools.partial(sum_kernel, n_energy, n_mom, scale),
        out_shape=jax.ShapeDtypeStruct(flow.shape, jnp.float32),
        in_specs=[vmem],
        out_specs=vmem,
        scratch_shapes=[
            pltpu.VMEM((n_mom,) + flow.shape, jnp.float32),
            pltpu.VMEM((n_energy, n_mom) + flow.shape, jnp.float32),
            pltpu.SemaphoreType.DMA,
            pltpu.SemaphoreType.DMA((copies,)),
            pltpu.SemaphoreType.DMA((copies,)),
        ],
        compiler_params=pltpu.CompilerParams(collective_id=0, has_side_effects=True),
        name="current_sum",
    )(flow)[0, 0]


def rotated(array, axis, by):
    size = lax.axis_size(axis)
    if by % size == 0:
        return array
    return lax.ppermute(array, axis, [(i, (i + by) % size) for i in range(size)])


def moved(field, by):
    count = field.shape[0]
    by = max(-count, min(count, by))
    blank = jnp.zeros_like(field[: abs(by)])
    if by > 0:
        return jnp.concatenate([field[by:], blank], 0)
    if by < 0:
        return jnp.concatenate([blank, field[:by]], 0)
    return field


def exchanged(amount, mean):
    n_energy = lax.axis_size("energy")
    here = lax.axis_index("energy")
    turns, rest = divmod(amount, n_energy)
    above = rotated(mean, "energy", -rest)
    below = rotated(mean, "energy", rest)
    upper = jnp.where(here + rest >= n_energy, moved(above, turns + 1), moved(above, turns))
    under = jnp.where(here - rest < 0, moved(below, -turns - 1), moved(below, -turns))
    return upper, under


def shards(lesser, greater, hamiltonian, coupling, shift, phonon_weight):
    n_energy = lax.axis_size("energy")
    n_mom = lax.axis_size("mom")
    here = lax.axis_index("energy")
    mine = lax.axis_index("mom")
    per_dev, slabs, width = lesser.shape[0], lesser.shape[3], lesser.shape[-1]
    total = per_dev * n_energy
    part = slabs // n_mom
    row = lax.broadcasted_iota(jnp.int32, (width, width), 0)
    col = lax.broadcasted_iota(jnp.int32, (width, width), 1)

    def share(x, owner):
        x = lax.dynamic_slice_in_dim(x[:, 0, 0], owner * part, part, 1)
        return jnp.where(row >= col, x[:, :, 1], x[:, :, 0])

    def reduced(x):
        mean = share(x, mine)
        for k in range(1, n_mom):
            mean = mean + rotated(share(x, (mine + k) % n_mom), "mom", k)
        return mean / n_mom

    def scattered(mean, up_weight, down_weight):
        upper, beneath = lax.switch(
            jnp.clip(shift[0] - 1, 0, SMAX - 1),
            [functools.partial(exchanged, p) for p in range(1, SMAX + 1)],
            mean,
        )
        return up_weight * upper + down_weight * beneath

    def gathered(own):
        sig = jnp.zeros((per_dev, slabs, width, width), jnp.float32)
        sig = lax.dynamic_update_slice_in_dim(sig, own, mine * part, 1)
        for k in range(1, n_mom):
            piece = rotated(own, "mom", k)
            sig = lax.dynamic_update_slice_in_dim(sig, piece, ((mine - k) % n_mom) * part, 1)
        return sig

    mean_less = reduced(lesser)
    mean_great = reduced(greater)
    own_less = scattered(mean_less, phonon_weight[0], phonon_weight[1])
    mean_great, own_less = lax.optimization_barrier((mean_great, own_less))
    sig_less = gathered(own_less)
    own_great = scattered(mean_great, phonon_weight[1], phonon_weight[0])
    sig_great = gathered(own_great)
    grid = (jnp.arange(per_dev) * n_energy + here).astype(jnp.float32)
    energy = (grid + 0.5) * (2.0 * band_edge / total) - band_edge
    scal = jnp.stack(
        [
            energy,
            jax.nn.sigmoid((left_level - energy) / thermal),
            jax.nn.sigmoid((right_level - energy) / thermal),
        ],
        0,
    )
    less_new, great_new, flowing = transport(
        scal, sig_less, sig_great, hamiltonian[0], coupling[0]
    )
    current = summed(flowing, 2.0 * band_edge / total)
    return (less_new[:, None, None], great_new[:, None, None], current)


def solution(mesh):
    block = P(None, "energy", "mom", None, None, None, None)
    return jax.shard_map(
        shards,
        mesh=mesh,
        in_specs=(block, block, P("mom"), P("mom"), P(), P()),
        out_specs=(block, block, P()),
        check_vma=False,
    )
```
